512 devices in a mesh: grp: 2 (over y), sp: 16 (over z), blk: 8 (over x), rep: 2 (over core).
Axes of the slice: x: 8, y: 2, z: 16, core: 2. Of those that a mesh axis runs over, the one named last changes fastest.
The devices are a block of a 8x8x16 slice.
Arguments:
- hidden: bfloat16 [16, 2048, 4096], P(('grp', 'blk'), 'sp'), parts along dimension 0, may hold values from -64 to 64
- queries: bfloat16 [16, 2048, 4096], P(('grp', 'blk'), 'sp', 'rep'), parts along dimension 0, may hold values from -600 to 600
- norm_gain: float32 [4096], replicated, may hold values from 0.1 to 1.9
- key_matrix: bfloat16 [4096, 1024], P('sp', 'rep'), may hold values from -0.09375 to 0.09375
- value_matrix: bfloat16 [4096, 1024], P('sp', 'rep'), may hold values from -0.09375 to 0.09375
- key_shift_bias: bfloat16 [1024], P('rep'), may hold values from -3 to 3
- value_shift_bias: bfloat16 [1024], P('rep'), may hold values from -3 to 3
- doc_lengths: int32 [16], P('grp'), parts along dimension 0, may hold values from 1 to 4097, 16384 in all
Outputs:
- attended: bfloat16 [16, 2048, 4096], P(('grp', 'blk'), 'sp', 'rep'), parts along dimension 0
The draws below stay inside these ranges and needn't reach their ends.
There are 2 independent parts, one for each index of `grp`. The reference program is written for one: setup_inputs(seed, part) draws one part's arguments, and reference() takes and returns one part's arrays. A program takes and returns all parts, laid end to end along the dimension named above; an argument that names none is the same for every part. Nothing has to cross between parts.
Inputs may be any that keep to these rules, and one draw needn't show every extreme that they name: `doc_lengths`: the lengths of the 8 documents packed in order into the sequence; they sum to 16384, and the longest is exactly 4097 tokens.
All inputs are finite; a program needn't handle non-finite values.
Results may differ from the reference program's by a relative error of at most 0.012.
The reference program's roundings to bfloat16 on the way count: a program that leaves them out, or rounds other values in their place, can miss the bound.
Values may be sent and summed in bfloat16 or wider, within the bound.
A program may use at most 64 MiB of HBM per device.

```python
import math
import jax
import jax.numpy as jnp
import numpy as np
from jax import lax

MODEL_WIDTH = 4096
QUERY_HEADS = 32
KEY_VALUE_HEADS = 8
HEAD_DIMENSION = 128
DOCS = 8
CH = 2048
SEQUENCE_TOKENS = 16384
DOC_MOST = 4097


def draw_queries(key, part):
    first_key = jax.random.fold_in(jax.random.fold_in(key, 11), 0)
    full_shape = (SEQUENCE_TOKENS // CH, CH, QUERY_HEADS * HEAD_DIMENSION)
    drawn = jnp.clip(jax.random.normal(first_key, full_shape, jnp.float32), -4.0, 4.0)
    return drawn.astype(jnp.bfloat16)


def draw_hidden(key, part):
    first_key = jax.random.fold_in(jax.random.fold_in(key, 23), 0)
    full_shape = (SEQUENCE_TOKENS // CH, CH, MODEL_WIDTH)
    drawn = jnp.clip(jax.random.normal(first_key, full_shape, jnp.float32), -5.0, 5.0)
    return drawn.astype(jnp.bfloat16)


def level_of(key, dims, cuts, smallest, high):
    def one(axis_at, blocks):
        heights = jax.random.uniform(jax.random.fold_in(jax.random.fold_in(key, 6), axis_at), (blocks,), jnp.float32, smallest / len(cuts), high / len(cuts))
        return jnp.repeat(jnp.exp(heights), dims[axis_at] // blocks).reshape((-1,) + (1,) * (len(dims) - axis_at - 1))

    level = one(*cuts[0])
    for cut in cuts[1:]:
        level = level * one(*cut)
    return level


def profile(amount, total, bound, slope):
    loads = [(1 << 20) // math.isqrt(standing ** slope) + 1 for standing in range(2, amount + 1)]
    spare, given = total - bound - (amount - 1), [1] * (amount - 1)
    while spare > 0:
        candidates = [i for i in range(amount - 1) if given[i] < bound]
        pool, remaining = sum([loads[i] for i in candidates]), spare
        for i in candidates:
            extra = min(bound - given[i], max(1, remaining * loads[i] // pool), spare)
            given[i] = given[i] + extra
            spare = spare - extra
    return np.array([bound] + given)


def ragged(stream_key, amount, total, most, skew):
    if amount == 2:
        one = jax.random.randint(stream_key, (), max(1, total - most), min(most, total - 1) + 1)
        return jnp.stack([one, total - one])
    tallies = jnp.asarray(profile(amount, total, most, skew), jnp.int32)
    couples = (amount - 1) // 2
    giver, receiver = tallies[1:1 + 2 * couples:2], tallies[2:2 + 2 * couples:2]
    room = jnp.minimum(giver - 1, most - receiver)
    shifted = jax.random.randint(jax.random.fold_in(stream_key, 1), (couples,), 0, 1 << 20) % (room + 1)
    tallies = tallies.at[1:1 + 2 * couples:2].set(giver - shifted).at[2:2 + 2 * couples:2].set(receiver + shifted)
    return tallies[jax.random.permutation(jax.random.fold_in(stream_key, 2), amount)]


def centred(own_key, extent, width, most, shards=(), dtype=jnp.bfloat16):
    loudness = level_of(own_key, extent, shards, -0.22, 0.18) if shards else 1.0
    entries = jax.random.normal(own_key, extent, jnp.float32) * width * loudness
    return jnp.minimum(jnp.maximum(entries, -most), most).astype(dtype)


def setup_inputs(seed: int = 0, part: int = 0) -> dict:
    key_list = jax.random.split(jax.random.key(seed), 9)
    own_keys = jax.random.split(jax.random.fold_in(key_list[8], part), 9)
    return {
        "hidden": draw_hidden(jax.random.fold_in(jax.random.fold_in(key_list[8], part), 71), part),
        "queries": draw_queries(jax.random.fold_in(jax.random.fold_in(key_list[8], part), 71), part),
        "norm_gain": jnp.clip(1.0 + 0.18 * jax.random.normal(key_list[2], (MODEL_WIDTH,), jnp.float32), 0.1, 1.9),
        "key_matrix": centred(key_list[3], (MODEL_WIDTH, KEY_VALUE_HEADS * HEAD_DIMENSION), MODEL_WIDTH ** -0.5, 0.09375, ((0, 16), (1, 2))),
        "value_matrix": centred(key_list[4], (MODEL_WIDTH, KEY_VALUE_HEADS * HEAD_DIMENSION), MODEL_WIDTH ** -0.5, 0.09375, ((0, 16), (1, 2))),
        "key_shift_bias": centred(key_list[5], (KEY_VALUE_HEADS * HEAD_DIMENSION,), 0.5, 3.0, ((0, 2),)),
        "value_shift_bias": centred(key_list[6], (KEY_VALUE_HEADS * HEAD_DIMENSION,), 0.5, 3.0, ((0, 2),)),
        "doc_lengths": ragged(own_keys[7], DOCS, SEQUENCE_TOKENS, DOC_MOST, 2).astype(jnp.int32),
    }


EPS_VALUE = 1e-06
THETA_BASE = 1000000.0

def apply_rotation(projected, token_places):
    half_size = projected.shape[-1] // 2
    freq_index = jnp.arange(half_size).astype(jnp.float32)
    inverse = jnp.exp(freq_index * (-2.0 * math.log(THETA_BASE) / projected.shape[-1]))
    angles = token_places[:, None] * inverse[None, :]
    cosine = jnp.cos(angles)[:, None, :]
    sine = jnp.sin(angles)[:, None, :]
    first_half = projected[..., :half_size]
    second_half = projected[..., half_size:]
    return jnp.concatenate([first_half * cosine - second_half * sine, second_half * cosine + first_half * sine], axis=-1)

def doc_index(token_places, doc_lengths):
    ending = jnp.cumsum(doc_lengths).astype(jnp.int32)
    return lax.optimization_barrier(jnp.sum((token_places[:, None] >= ending[None, :]).astype(jnp.int32), axis=1))

def reference(hidden, queries, norm_gain, key_matrix, value_matrix, key_shift_bias, value_shift_bias, doc_lengths):
    rows_all = hidden.reshape(SEQUENCE_TOKENS, MODEL_WIDTH).astype(jnp.float32)
    row_scale = lax.rsqrt(lax.optimization_barrier(jnp.mean(rows_all * rows_all, axis=1, keepdims=True)) + EPS_VALUE)
    normed = (rows_all * row_scale * norm_gain.astype(jnp.float32)).astype(jnp.bfloat16)
    token_places = jnp.arange(SEQUENCE_TOKENS).astype(jnp.int32)
    key_projector = jnp.dot(normed, key_matrix, preferred_element_type=jnp.float32) + key_shift_bias.astype(jnp.float32)
    value_projector = jnp.dot(normed, value_matrix, preferred_element_type=jnp.float32) + value_shift_bias.astype(jnp.float32)
    key_vectors = apply_rotation(key_projector.reshape(SEQUENCE_TOKENS, KEY_VALUE_HEADS, HEAD_DIMENSION), token_places.astype(jnp.float32)).astype(jnp.bfloat16)
    value_vectors = value_projector.reshape(SEQUENCE_TOKENS, KEY_VALUE_HEADS, HEAD_DIMENSION).astype(jnp.bfloat16)
    segment = doc_index(token_places, doc_lengths)
    visible = (token_places[None, :] <= token_places[:, None]) & (segment[None, :] == segment[:, None])
    query_heads = queries.reshape(SEQUENCE_TOKENS, QUERY_HEADS, HEAD_DIMENSION).transpose(1, 0, 2)
    heads_of_keys = jnp.repeat(key_vectors.transpose(1, 0, 2), QUERY_HEADS // KEY_VALUE_HEADS, axis=0)
    heads_of_values = jnp.repeat(value_vectors.transpose(1, 0, 2), QUERY_HEADS // KEY_VALUE_HEADS, axis=0)
    scale_factor = 1.0 / math.sqrt(HEAD_DIMENSION)

    def one_head(triple):
        query_rows, key_rows, value_rows = triple
        scores = jnp.dot(query_rows, key_rows.T, preferred_element_type=jnp.float32) * scale_factor
        scores = jnp.where(visible, scores, -1e+30)
        largest = lax.optimization_barrier(jnp.max(scores, axis=1, keepdims=True))
        weights = jnp.where(visible, jnp.exp(scores - largest), 0.0).astype(jnp.bfloat16)
        total = lax.optimization_barrier(jnp.sum(weights.astype(jnp.float32), axis=1, keepdims=True))
        summed = jnp.dot(weights, value_rows, preferred_element_type=jnp.float32)
        return (summed / total).astype(jnp.bfloat16)
    result = lax.map(one_head, (query_heads, heads_of_keys, heads_of_values))
    return result.transpose(1, 0, 2).reshape(SEQUENCE_TOKENS // CH, CH, QUERY_HEADS * HEAD_DIMENSION)
```

```python
import functools
import math

import jax
import jax.numpy as jnp
from jax import lax
from jax.experimental import pallas as pl
from jax.experimental.pallas import tpu as pltpu
from jax.sharding import PartitionSpec as P

HEAD = 128
EPS_VALUE = 1e-06
THETA_BASE = 1000000.0
NEG_FILL = -1e30
TILE = 512
MESH = pl.DeviceIdType.MESH
F32 = jnp.float32
BF16 = jnp.bfloat16


def ring_offsets(n):
    order = [0]
    for k in range(1, n // 2):
        order += [-k, k]
    return order + [n // 2]


def body(
    NZ, NX,
    ends, hidden, queries, gain, w_own, w_give, bias, cos_t, sin_t,
    out,
    wbuf, hbuf, nbuf, acc, kvown, qbuf, buf, obuf,
    pair_s, pair_r, own_s, zs, zr, xs, xr, hs, hr, gs, gr, qs, qr,
    ks, kr, ds, dr, fs, fr, os, orr,
):
    NP = NZ // 2
    ZH, XH = NP // 2, NX // 2
    z = lax.axis_index("sp")
    x = lax.axis_index("blk")
    r = lax.axis_index("rep")
    p = z // 2
    b = lax.rem(z, 2)
    rows = hidden.shape[0]
    half = rows // 2

    def mod(a, n):
        return lax.rem(a + 2 * n, n)

    def at(sp=None, blk=None, rep=None):
        return {
            "sp": z if sp is None else sp,
            "blk": x if blk is None else blk,
            "rep": r if rep is None else rep,
        }

    def remote(src, dst, ss, rs, dev):
        return pltpu.make_async_remote_copy(
            src_ref=src, dst_ref=dst, send_sem=ss, recv_sem=rs,
            device_id=dev, device_id_type=MESH,
        )

    barrier = pltpu.get_barrier_semaphore()
    for j in range(1, 2 * NZ):
        other = mod(2 * z + r + j, 2 * NZ)
        pl.semaphore_signal(
            barrier, inc=1, device_id=at(sp=other // 2, rep=lax.rem(other, 2)),
            device_id_type=MESH,
        )
    for dx in (1, -1):
        pl.semaphore_signal(
            barrier, inc=1, device_id=at(blk=mod(x + dx, NX)), device_id_type=MESH
        )
    pl.semaphore_wait(barrier, 2 * NZ + 1)

    slice_rows = wbuf.shape[3]
    mine = pl.ds(pl.multiple_of(x * slice_rows, slice_rows), slice_rows)
    partner = z + 1 - 2 * b

    give = remote(w_give.at[mine], wbuf.at[p, b, x], pair_s, pair_r, at(sp=partner))
    give.start()
    own = pltpu.make_async_copy(w_own.at[mine], wbuf.at[p, b, x], own_s)
    own.start()

    def z_send(h, d):
        item = mod(p - (h - 1) if d == 0 else p + (h - 1), NP)
        ref = wbuf.at[item, :, x] if h < ZH else wbuf.at[item, d, x]
        to = mod(z + 2 if d == 0 else z - 2, NZ)
        return remote(ref, ref, zs.at[d, h - 1], zr.at[d, h - 1], at(sp=to))

    def z_recv(h, d):
        item = mod(p - h if d == 0 else p + h, NP)
        ref = wbuf.at[item, :, x] if h < ZH else wbuf.at[item, d, x]
        return remote(ref, ref, zs.at[d, h - 1], zr.at[d, h - 1], at(sp=mod(z + 2, NZ)))

    offs = ring_offsets(NP)

    def x_send(i, h, d):
        item = mod(p + offs[i], NP)
        sl = mod(x - (h - 1) if d == 0 else x + (h - 1), NX)
        ref = wbuf.at[item, :, sl] if h < XH else wbuf.at[item, d, sl]
        to = mod(x + 1 if d == 0 else x - 1, NX)
        return remote(ref, ref, xs.at[i, d, h - 1], xr.at[i, d, h - 1], at(blk=to))

    def x_recv(i, h, d):
        item = mod(p + offs[i], NP)
        sl = mod(x - h if d == 0 else x + h, NX)
        ref = wbuf.at[item, :, sl] if h < XH else wbuf.at[item, d, sl]
        return remote(ref, ref, xs.at[i, d, h - 1], xr.at[i, d, h - 1], at(blk=mod(x + 1, NX)))

    HC = hs.shape[0]
    hrows = half // HC

    def h_send(k):
        ref_rows = pl.ds(pl.multiple_of(r * half + k * hrows, hrows), hrows)
        return remote(hidden.at[ref_rows], hbuf.at[ref_rows], hs.at[k], hr.at[k], at(sp=partner))

    def h_relay(k):
        ref_rows = pl.ds(pl.multiple_of(r * half + k * hrows, hrows), hrows)
        return remote(hbuf.at[ref_rows], hbuf.at[ref_rows], gs.at[k], gr.at[k], at(rep=1 - r))

    def h_relayed(k):
        ref_rows = pl.ds(pl.multiple_of((1 - r) * half + k * hrows, hrows), hrows)
        return remote(hbuf.at[ref_rows], hbuf.at[ref_rows], gs.at[k], gr.at[k], at(rep=1 - r))

    QN = queries.shape[1] // HEAD

    def start_q(j):
        hl = mod(2 * lax.rem(p, QN // 2) + j, QN)
        dz = r * (QN // 2) + hl // 2
        dc = lax.rem(hl, 2)
        src = queries.at[:, pl.ds(pl.multiple_of(hl * HEAD, HEAD), HEAD)]
        dst = qbuf.at[pl.ds(pl.multiple_of(z * rows, rows), rows)]
        self_case = (dz == z) & (dc == r)

        @pl.when(self_case)
        def _():
            pltpu.make_async_copy(src, dst, qr.at[z]).start()

        @pl.when(jnp.logical_not(self_case))
        def _():
            remote(src, dst, qs.at[j], qr.at[z], at(sp=dz, rep=dc)).start()

    def finish_q_send(j):
        hl = mod(2 * lax.rem(p, QN // 2) + j, QN)
        dz = r * (QN // 2) + hl // 2
        dc = lax.rem(hl, 2)
        src = queries.at[:, pl.ds(pl.multiple_of(hl * HEAD, HEAD), HEAD)]
        dst = qbuf.at[pl.ds(pl.multiple_of(z * rows, rows), rows)]

        @pl.when(jnp.logical_not((dz == z) & (dc == r)))
        def _():
            remote(src, dst, qs.at[j], qr.at[z], at(sp=dz, rep=dc)).wait_send()

    def norm_into(src, row0):
        step = 16

        def one(k, _):
            at_rows = pl.ds(pl.multiple_of(k * step, step), step)
            v = src[at_rows, :].astype(F32)
            scale = lax.rsqrt(jnp.mean(v * v, axis=1, keepdims=True) + EPS_VALUE)
            nbuf[pl.ds(pl.multiple_of(row0 + k * step, step), step), :] = (
                v * scale * gain[...]
            ).astype(BF16)
            return 0

        lax.fori_loop(0, rows // step, one, 0)

    WK = wbuf.shape[1] * wbuf.shape[2] * wbuf.shape[3]

    def dot_item(i, first):
        item = mod(p + offs[i], NP)
        lhs = nbuf[:, pl.ds(pl.multiple_of(item * WK, WK), WK)]
        w = wbuf[item].reshape(WK, wbuf.shape[4])
        d = jnp.dot(lhs, w, preferred_element_type=F32)
        if first:
            acc[...] = d
        else:
            acc[...] += d

    own.wait()
    give.wait_recv()
    last = NP + XH - 1
    done_dots = 0
    q_next = 0
    for t in range(last + 1):
        if t < ZH:
            for d in (0, 1):
                if t:
                    z_recv(t, d).wait_recv()
                z_send(t + 1, d).start()
        elif t == ZH:
            for d in (0, 1):
                z_recv(ZH, d).wait_recv()
        for h in range(1, XH + 1):
            i = t - (h - 1)
            if 0 <= i < NP:
                for d in (0, 1):
                    if h > 1:
                        x_recv(i, h - 1, d).wait_recv()
                    x_send(i, h, d).start()
        if t < HC:
            h_send(t).start()
        if t == 0:
            norm_into(hidden, b * rows)
        if 1 <= t <= HC:
            h_send(t - 1).wait_recv()
            h_relay(t - 1).start()
        if t >= 1:
            for _ in range(3):
                if q_next < QN:
                    start_q(q_next)
                    q_next += 1
        if t == HC + 2:
            for k in range(HC):
                h_relayed(k).wait_recv()
            norm_into(hbuf, (1 - b) * rows)
        if t >= HC + 3:
            while done_dots + XH <= t:
                for d in (0, 1):
                    x_recv(done_dots, XH, d).wait_recv()
                dot_item(done_dots, done_dots == 0)
                done_dots += 1
    while q_next < QN:
        start_q(q_next)
        q_next += 1
    while done_dots < NP:
        for d in (0, 1):
            x_recv(done_dots, XH, d).wait_recv()
        dot_item(done_dots, done_dots == 0)
        done_dots += 1

    NH = kvown.shape[0]
    for j in range(NH):
        cols = slice(j * HEAD, (j + 1) * HEAD)
        y = acc[:, cols] + bias[:, cols]
        kvown[j] = (y * cos_t[...] + pltpu.roll(y, HEAD // 2, 1) * sin_t[...]).astype(BF16)

    g = z // 2

    def start_kv(k):
        k2 = mod(k + 2 * lax.rem(p, NH), 2 * NH)
        j, e = k2 // 2, lax.rem(k2, 2)
        dz = 2 * (NH * r + j) + e
        src = kvown.at[j]
        dst = buf.at[b, 2 * NP + p]
        self_case = (dz == z) & (b == r)

        @pl.when(self_case)
        def _():
            pltpu.make_async_copy(src, dst, kr.at[p]).start()

        @pl.when(jnp.logical_not(self_case))
        def _():
            remote(src, dst, ks.at[k], kr.at[p], at(sp=dz, rep=b)).start()

    def finish_kv_send(k):
        k2 = mod(k + 2 * lax.rem(p, NH), 2 * NH)
        j, e = k2 // 2, lax.rem(k2, 2)
        dz = 2 * (NH * r + j) + e

        @pl.when(jnp.logical_not((dz == z) & (b == r)))
        def _():
            remote(kvown.at[j], buf.at[b, 2 * NP + p], ks.at[k], kr.at[p], at(sp=dz, rep=b)).wait_send()

    for k in range(2 * NH):
        start_kv(k)

    def relay(a, i):
        q = mod(g + offs[i], NP)
        here = buf.at[r, (2 - a) * NP + q]
        if a == 0:
            remote(here, here, ks.at[0], kr.at[q], at()).wait_recv()
        else:
            remote(here, here, fs.at[a - 1, i], fr.at[a - 1, i], at()).wait_recv()
        remote(here, here, ds.at[a, i], dr.at[a, i], at(rep=1 - r)).start()
        if a < 2:
            there = buf.at[r, (1 - a) * NP + q]
            remote(here, there, fs.at[a, i], fr.at[a, i], at(blk=mod(x + 1, NX))).start()

    def relayed(a, i):
        q = mod(g + offs[i], NP)
        ref = buf.at[1 - r, (2 - a) * NP + q]
        remote(ref, ref, ds.at[a, i], dr.at[a, i], at(rep=1 - r)).wait_recv()

    for i in range(NP):
        relay(0, i)
    for a in (1, 2):
        for i in range(NP):
            relay(a, i)
    for a in (0, 1, 2):
        for i in range(NP):
            relayed(a, i)
    for zz in range(NZ):
        ref = qbuf.at[pl.ds(zz * rows, rows)]
        remote(ref, ref, qs.at[0], qr.at[zz], at()).wait_recv()

    NT = qbuf.shape[0] // TILE
    per = TILE // rows
    span = qbuf.shape[0]
    units = TILE // buf.shape[2]
    factor = math.log2(math.e) / math.sqrt(HEAD)
    ones = jnp.ones((TILE, HEAD), BF16)
    col = lax.broadcasted_iota(jnp.int32, (TILE, TILE), 1)
    row = lax.broadcasted_iota(jnp.int32, (TILE, TILE), 0)
    oc = z // (NZ // 2)
    olane = lax.rem(2 * z + r, QN)

    def out_copy(qi, k):
        dz = qi * per + k
        src = obuf.at[qi, pl.ds(k * rows, rows)]
        dst = out.at[:, pl.ds(pl.multiple_of(olane * HEAD, HEAD), HEAD)]
        return dz, src, dst, (dz == z) & (oc == r)

    def q_tile(n, _):
        shift = jnp.where(n == 0, 2, jnp.where(n == 1, 1, jnp.where(n == 2, 3, 0)))
        qi = lax.rem(z // per + shift, NT)
        q = qbuf[pl.ds(pl.multiple_of(qi * TILE, TILE), TILE), :]
        pos = x * span + qi * TILE + lax.broadcasted_iota(jnp.int32, (TILE, HEAD), 0)
        lo = jnp.zeros((TILE, HEAD), jnp.int32)
        for d in range(ends.shape[0]):
            lo = jnp.where(pos >= ends[d], ends[d], lo)
        m = None
        for back in range(2 * NT + 1):
            tile = 2 * NT + qi - back
            kk = buf[0, pl.ds(tile * units, units)].reshape(TILE, HEAD)
            vv = buf[1, pl.ds(tile * units, units)].reshape(TILE, HEAD)
            s = lax.dot_general(q, kk, (((1,), (1,)), ((), ())), preferred_element_type=F32)
            base = x * span + (qi - back) * TILE
            low = jnp.concatenate([lo - base] * (TILE // HEAD), axis=1)
            seen = col >= low
            if back == 0:
                seen = seen & (col <= row)
            s = jnp.where(seen, s, NEG_FILL)
            top = jnp.broadcast_to(jnp.max(s, axis=1, keepdims=True), (TILE, HEAD))
            m_new = top if m is None else jnp.maximum(m, top)
            w = jnp.exp2(
                (s - jnp.concatenate([m_new] * (TILE // HEAD), axis=1)) * factor
            ).astype(BF16)
            pv = jnp.dot(w, jnp.concatenate([vv, ones], axis=1), preferred_element_type=F32)
            if m is None:
                total = pv
            else:
                alpha = jnp.exp2((m - m_new) * factor)
                total = total * jnp.concatenate([alpha, alpha], axis=1) + pv
            m = m_new
        obuf[qi] = (total[:, :HEAD] / total[:, HEAD:]).astype(BF16)
        for k in range(per):
            dz, src, dst, self_case = out_copy(qi, k)

            @pl.when(self_case)
            def _():
                pltpu.make_async_copy(src, dst, orr.at[olane]).start()

            @pl.when(jnp.logical_not(self_case))
            def _():
                remote(src, dst, os.at[qi, k], orr.at[olane], at(sp=dz, rep=oc)).start()

        return 0

    lax.fori_loop(0, NT, q_tile, 0)

    for hl in range(QN):
        ref = out.at[:, pl.ds(hl * HEAD, HEAD)]
        remote(ref, ref, os.at[0, 0], orr.at[hl], at()).wait_recv()
    for qi in range(NT):
        for k in range(per):
            dz, src, dst, self_case = out_copy(qi, k)

            @pl.when(jnp.logical_not(self_case))
            def _():
                remote(src, dst, os.at[qi, k], orr.at[olane], at(sp=dz, rep=oc)).wait_send()

    give.wait_send()
    for h in range(1, ZH + 1):
        for d in (0, 1):
            z_send(h, d).wait_send()
    for i in range(NP):
        for h in range(1, XH + 1):
            for d in (0, 1):
                x_send(i, h, d).wait_send()
    for k in range(HC):
        h_send(k).wait_send()
        h_relay(k).wait_send()
    for j in range(QN):
        finish_q_send(j)
    for k in range(2 * NH):
        finish_kv_send(k)
    for a in (0, 1, 2):
        for i in range(NP):
            q = mod(g + offs[i], NP)
            here = buf.at[r, (2 - a) * NP + q]
            remote(here, here, ds.at[a, i], dr.at[a, i], at(rep=1 - r)).wait_send()
            if a < 2:
                remote(here, here, fs.at[a, i], fr.at[a, i], at()).wait_send()


def on_device(
    hidden, queries, norm_gain, key_matrix, value_matrix, key_shift_bias, value_shift_bias,
    doc_lengths,
):
    NZ, NX = lax.axis_size("sp"), lax.axis_size("blk")
    NP = NZ // 2
    z, x = lax.axis_index("sp"), lax.axis_index("blk")
    rows, width = hidden.shape[1:]
    span = rows * NZ
    krows, kcols = key_matrix.shape
    heads = kcols // HEAD
    even = lax.rem(z, 2) == 0
    w_own = jnp.where(even, key_matrix, value_matrix)
    w_give = jnp.where(even, value_matrix, key_matrix)
    bias = jnp.where(even, key_shift_bias, value_shift_bias).astype(F32)[None]
    places = (x * span + (z // 2) * 2 * rows + jnp.arange(2 * rows)).astype(F32)
    freq = jnp.arange(HEAD // 2).astype(F32)
    inverse = jnp.exp(freq * (-2.0 * math.log(THETA_BASE) / HEAD))
    angles = places[:, None] * inverse[None, :]
    cosine, sine = jnp.cos(angles), jnp.sin(angles)
    cos_t = jnp.where(even, jnp.concatenate([cosine, cosine], 1), 1.0)
    sin_t = jnp.where(even, jnp.concatenate([-sine, sine], 1), 0.0)
    ends = jnp.cumsum(doc_lengths).astype(jnp.int32)
    HC = 4
    QN = queries.shape[2] // HEAD
    NT = span // TILE
    dma = pltpu.SemaphoreType.DMA
    vmem = pl.BlockSpec(memory_space=pltpu.VMEM)
    out = pl.pallas_call(
        functools.partial(body, NZ, NX),
        out_shape=jax.ShapeDtypeStruct((rows, queries.shape[2]), BF16),
        in_specs=[pl.BlockSpec(memory_space=pltpu.SMEM)] + [vmem] * 8,
        out_specs=vmem,
        scratch_shapes=[
            pltpu.VMEM((NP, 2, NX, krows // NX, kcols), BF16),
            pltpu.VMEM((rows, width), BF16),
            pltpu.VMEM((2 * rows, width), BF16),
            pltpu.VMEM((2 * rows, kcols), F32),
            pltpu.VMEM((heads, 2 * rows, HEAD), BF16),
            pltpu.VMEM((span, HEAD), BF16),
            pltpu.VMEM((2, 3 * NP, 2 * rows, HEAD), BF16),
            pltpu.VMEM((NT, TILE, HEAD), BF16),
            dma(()), dma(()), dma(()),
            dma((2, NP // 2)), dma((2, NP // 2)),
            dma((NP, 2, NX // 2)), dma((NP, 2, NX // 2)),
            dma((HC,)), dma((HC,)), dma((HC,)), dma((HC,)),
            dma((QN,)), dma((NZ,)),
            dma((2 * heads,)), dma((NP,)),
            dma((3, NP)), dma((3, NP)),
            dma((2, NP)), dma((2, NP)),
            dma((NT, TILE // rows)), dma((QN,)),
        ],
        compiler_params=pltpu.CompilerParams(
            collective_id=0, has_side_effects=True, vmem_limit_bytes=56 * 2**20
        ),
    )(
        ends, hidden[0], queries[0], norm_gain[None].astype(F32), w_own, w_give, bias,
        cos_t, sin_t,
    )
    return out[None]


def solution(mesh):
    in_specs = (
        P(("grp", "blk"), "sp", None),
        P(("grp", "blk"), "sp", "rep"),
        P(),
        P("sp", "rep"),
        P("sp", "rep"),
        P("rep"),
        P("rep"),
        P("grp"),
    )
    out_specs = P(("grp", "blk"), "sp", "rep")
    return jax.shard_map(
        on_device, mesh=mesh, in_specs=in_specs, out_specs=out_specs, check_vma=False
    )
```

```python
import functools
import math

import jax
import jax.numpy as jnp
from jax import lax
from jax.experimental import pallas as pl
from jax.experimental.pallas import tpu as pltpu
from jax.sharding import PartitionSpec as P

HEAD = 128
EPS_VALUE = 1e-06
THETA_BASE = 1000000.0
NEG_FILL = -1e30
KEY_TILE = 512
MESH = pl.DeviceIdType.MESH
F32 = jnp.float32
BF16 = jnp.bfloat16


def ring_offsets(n):
    order = [0]
    for k in range(1, n // 2):
        order += [-k, k]
    return order + [n // 2]


def body(
    NZ, NX,
    lengths, hidden, queries, gain, wk, wv, bias, cos_t, sin_t,
    out,
    wbuf, hown, hbuf, nbuf, acc, kvown, qbuf, buf, obuf,
    pair_s, pair_r, own_s, hown_s, zs, zr, xs, xr, hs, hr, gs, gr, qs, qr,
    ks, kr, ds, dr, fs, fr, os, orr,
):
    NP = NZ // 2
    ZH, XH = NP // 2, NX // 2
    z = lax.axis_index("sp")
    x = lax.axis_index("blk")
    r = lax.axis_index("rep")
    p = z // 2
    b = lax.rem(z, 2)
    rows = hidden.shape[0]
    half = rows // 2

    def mod(a, n):
        return lax.rem(a + 2 * n, n)

    def at(sp=None, blk=None, rep=None):
        return {
            "sp": z if sp is None else sp,
            "blk": x if blk is None else blk,
            "rep": r if rep is None else rep,
        }

    def remote(src, dst, ss, rs, dev):
        return pltpu.make_async_remote_copy(
            src_ref=src, dst_ref=dst, send_sem=ss, recv_sem=rs,
            device_id=dev, device_id_type=MESH,
        )

    def drain(ref, sem):
        pltpu.make_async_copy(ref, ref, sem).wait()

    def signal(sem, dev):
        pl.semaphore_signal(sem, inc=1, device_id=dev, device_id_type=MESH)

    barrier = pltpu.get_barrier_semaphore()
    for j in range(1, 2 * NZ):
        other = mod(2 * z + r + j, 2 * NZ)
        signal(barrier, at(sp=other // 2, rep=lax.rem(other, 2)))
    for dx in (1, -1):
        signal(barrier, at(blk=mod(x + dx, NX)))

    slice_rows = wbuf.shape[3]
    mine = pl.ds(pl.multiple_of(x * slice_rows, slice_rows), slice_rows)
    partner = z + 1 - 2 * b
    own_slot = wbuf.at[p, b, x]

    @pl.when(b == 0)
    def _():
        pltpu.make_async_copy(wk.at[mine], own_slot, own_s).start()

    @pl.when(b == 1)
    def _():
        pltpu.make_async_copy(wv.at[mine], own_slot, own_s).start()

    pltpu.make_async_copy(hidden, hown, hown_s).start()
    pl.semaphore_wait(barrier, 2 * NZ + 1)

    @pl.when(b == 0)
    def _():
        remote(wv.at[mine], own_slot, pair_s, pair_r, at(sp=partner)).start()

    @pl.when(b == 1)
    def _():
        remote(wk.at[mine], own_slot, pair_s, pair_r, at(sp=partner)).start()

    give = remote(wk.at[mine], own_slot, pair_s, pair_r, at(sp=partner))

    items = [mod(p + o, NP) for o in ring_offsets(NP)]

    def z_send(h, d):
        item = mod(p - (h - 1) if d == 0 else p + (h - 1), NP)
        ref = wbuf.at[item, :, x] if h < ZH else wbuf.at[item, d, x]
        to = mod(z + 2 if d == 0 else z - 2, NZ)
        return remote(ref, ref, zs, zr.at[d, h - 1], at(sp=to))

    def z_recv(h, d):
        item = mod(p - h if d == 0 else p + h, NP)
        ref = wbuf.at[item, :, x] if h < ZH else wbuf.at[item, d, x]
        return remote(ref, ref, zs, zr.at[d, h - 1], at(sp=mod(z + 2, NZ)))

    def x_send(i, h, d):
        sl = mod(x - (h - 1) if d == 0 else x + (h - 1), NX)
        ref = wbuf.at[items[i], :, sl] if h < XH else wbuf.at[items[i], d, sl]
        to = mod(x + 1 if d == 0 else x - 1, NX)
        return remote(ref, ref, xs, xr.at[i, d, h - 1], at(blk=to))

    def x_recv(i, h, d):
        sl = mod(x - h if d == 0 else x + h, NX)
        ref = wbuf.at[items[i], :, sl] if h < XH else wbuf.at[items[i], d, sl]
        return remote(ref, ref, xs, xr.at[i, d, h - 1], at(blk=mod(x + 1, NX)))

    HC = hr.shape[0]
    hrows = half // HC

    def h_send(k):
        ref_rows = pl.ds(pl.multiple_of(r * half + k * hrows, hrows), hrows)
        return remote(hidden.at[ref_rows], hbuf.at[ref_rows], hs, hr.at[k], at(sp=partner))

    def h_relay(k):
        ref_rows = pl.ds(pl.multiple_of(r * half + k * hrows, hrows), hrows)
        return remote(hbuf.at[ref_rows], hbuf.at[ref_rows], gs, gr, at(rep=1 - r))

    QN = queries.shape[1] // HEAD

    def q_case(j):
        hl = mod(2 * lax.rem(p, QN // 2) + j, QN)
        dz = r * (QN // 2) + hl // 2
        dc = lax.rem(hl, 2)
        src = queries.at[:, pl.ds(pl.multiple_of(hl * HEAD, HEAD), HEAD)]
        dst = qbuf.at[pl.ds(pl.multiple_of(z * rows, rows), rows)]
        return src, dst, at(sp=dz, rep=dc), (dz == z) & (dc == r)

    def start_q(j):
        src, dst, dev, self_case = q_case(j)

        @pl.when(self_case)
        def _():
            pltpu.make_async_copy(src, dst, qr).start()

        @pl.when(jnp.logical_not(self_case))
        def _():
            remote(src, dst, qs, qr, dev).start()

    def norm_into(src, row0):
        step = 16

        def one(k, _):
            at_rows = pl.ds(pl.multiple_of(k * step, step), step)
            v = src[at_rows, :].astype(F32)
            scale = lax.rsqrt(jnp.mean(v * v, axis=1, keepdims=True) + EPS_VALUE)
            nbuf[pl.ds(pl.multiple_of(row0 + k * step, step), step), :] = (
                v * scale * gain[...]
            ).astype(BF16)
            return 0

        lax.fori_loop(0, rows // step, one, 0)

    WK = wbuf.shape[1] * wbuf.shape[2] * wbuf.shape[3]

    def dot_item(i, first):
        lhs = nbuf[:, pl.ds(pl.multiple_of(items[i] * WK, WK), WK)]
        w = wbuf[items[i]].reshape(WK, wbuf.shape[4])
        d = jnp.dot(lhs, w, preferred_element_type=F32)
        if first:
            acc[...] = d
        else:
            acc[...] += d

    pltpu.make_async_copy(wk.at[mine], own_slot, own_s).wait()
    give.wait_recv()
    last = NP + XH - 1
    done_dots = 0
    q_next = 0
    q_ticks = [0] * (last + 1)
    for n in range(QN):
        q_ticks[min(ZH + n // 3, last)] += 1
    for t in range(last + 1):
        with jax.named_scope(f"t{t}"):
            for h in range(XH, 0, -1):
                if h == 1:
                    if 1 <= t <= ZH:
                        for d in (0, 1):
                            z_recv(t, d).wait_recv()
                    if t < ZH:
                        for d in (0, 1):
                            z_send(t + 1, d).start()
                i = t - (h - 1)
                if 0 <= i < NP:
                    for d in (0, 1):
                        if h > 1:
                            x_recv(i, h - 1, d).wait_recv()
                        x_send(i, h, d).start()
            if t < HC:
                h_send(t).start()
            if t == 0:
                pltpu.make_async_copy(hidden, hown, hown_s).wait()
                norm_into(hown, b * rows)
            for _ in range(q_ticks[t]):
                start_q(q_next)
                q_next += 1
            if 3 <= t < HC + 3:
                h_send(t - 3).wait_recv()
                h_relay(t - 3).start()
            if t == HC + 4:
                drain(hbuf.at[pl.ds(pl.multiple_of((1 - r) * half, half), half)], gr)
                norm_into(hbuf, (1 - b) * rows)
            if t >= HC + 4:
                for _ in range(2 if t < last else NP):
                    if done_dots < NP and done_dots + XH <= t:
                        for d in (0, 1):
                            x_recv(done_dots, XH, d).wait_recv()
                        dot_item(done_dots, done_dots == 0)
                        done_dots += 1
    assert done_dots == NP and q_next == QN

    NH = kvown.shape[0]
    for j in range(NH):
        cols = slice(j * HEAD, (j + 1) * HEAD)

        @pl.when(b == 0)
        def _():
            y = acc[:, cols] + bias[0:1, cols]
            kvown[j] = (y * cos_t[...] + pltpu.roll(y, HEAD // 2, 1) * sin_t[...]).astype(BF16)

        @pl.when(b == 1)
        def _():
            kvown[j] = (acc[:, cols] + bias[1:2, cols]).astype(BF16)

    prow = 2 * rows
    span = rows * NZ

    def unit(a, q):
        return pl.ds(pl.multiple_of((2 - a) * span + q * prow, prow), prow)

    def kv_case(k):
        j, e = lax.rem(k // 2 + p, NH), k % 2
        dz = 2 * (NH * r + j) + e
        return kvown.at[j], buf.at[b, unit(0, p)], at(sp=dz, rep=b), (dz == z) & (b == r)

    def start_kv(k):
        src, dst, dev, self_case = kv_case(k)

        @pl.when(self_case)
        def _():
            pltpu.make_async_copy(src, dst, kr.at[p]).start()

        @pl.when(jnp.logical_not(self_case))
        def _():
            remote(src, dst, ks, kr.at[p], dev).start()

    for k in range(2 * NH):
        start_kv(k)

    def relay(a, q):
        here = buf.at[r, unit(a, q)]
        if a == 0:
            remote(here, here, ks, kr.at[q], at()).wait_recv()
        else:
            remote(here, here, fs, fr.at[a - 1, q], at()).wait_recv()
        remote(here, here, ds, dr, at(rep=1 - r)).start()
        if a < 2:
            there = buf.at[r, unit(a + 1, q)]
            remote(here, there, fs, fr.at[a, q], at(blk=mod(x + 1, NX))).start()

    pairs = []
    for k in range(NH):
        first = mod(p - k, NH)
        pairs += [first + NH * c for c in range(NP // NH)]
    for i in range(NP + 2):
        with jax.named_scope(f"relay{i}"):
            for a in (0, 1, 2):
                if 0 <= i - a < NP:
                    relay(a, pairs[i - a])
    with jax.named_scope("relayed"):
        drain(buf.at[1 - r], dr)
        drain(qbuf, qr)

    KT = KEY_TILE // rows
    factor = math.log2(math.e) / math.sqrt(HEAD)
    ones = jnp.ones((KEY_TILE, HEAD), BF16)
    oc = z // (NZ // 2)
    olane = lax.rem(2 * z + r, QN)
    odst = out.at[:, pl.ds(pl.multiple_of(olane * HEAD, HEAD), HEAD)]

    def q_tile(qi):
        q = qbuf[pl.ds(pl.multiple_of(qi * rows, rows), rows), :]
        first = x * span + qi * rows
        pos = first + lax.broadcasted_iota(jnp.int32, (rows, HEAD), 0)
        lo = jnp.zeros((rows, HEAD), jnp.int32)
        end = jnp.int32(0)
        for d in range(lengths.shape[0]):
            end = end + lengths[d]
            lo = jnp.where(pos >= end, end, lo)
        lo = lo - first
        m = None
        for back in range(2 * NZ // KT + 1):
            n = rows if back == 0 else KEY_TILE
            at_rows = pl.ds(pl.multiple_of(2 * span + qi * rows - back * KEY_TILE, rows), n)
            s = lax.dot_general(
                q, buf[0, at_rows, :], (((1,), (1,)), ((), ())), preferred_element_type=F32
            )
            col = lax.broadcasted_iota(jnp.int32, (rows, n), 1)
            low = lo + back * KEY_TILE
            seen = col >= jnp.concatenate([low] * (n // HEAD), axis=1)
            if back == 0:
                seen = seen & (col <= lax.broadcasted_iota(jnp.int32, (rows, n), 0))
            s = jnp.where(seen, s, NEG_FILL)
            top = jnp.broadcast_to(jnp.max(s, axis=1, keepdims=True), (rows, HEAD))
            m_new = top if m is None else jnp.maximum(m, top)
            w = jnp.exp2((s - jnp.concatenate([m_new] * (n // HEAD), axis=1)) * factor).astype(BF16)
            vv = jnp.concatenate([buf[1, at_rows, :], ones[:n]], axis=1)
            pv = jnp.dot(w, vv, preferred_element_type=F32)
            if m is None:
                total = pv
            else:
                alpha = jnp.exp2((m - m_new) * factor)
                total = total * jnp.concatenate([alpha, alpha], axis=1) + pv
            m = m_new
        obuf[pl.ds(pl.multiple_of(qi * rows, rows), rows), :] = (
            total[:, :HEAD] / total[:, HEAD:]
        ).astype(BF16)

    def send_out(dz):
        src = obuf.at[pl.ds(pl.multiple_of(dz * rows, rows), rows)]
        self_case = (dz == z) & (oc == r)

        @pl.when(self_case)
        def _():
            pltpu.make_async_copy(src, odst, orr).start()

        @pl.when(jnp.logical_not(self_case))
        def _():
            remote(src, odst, os, orr, at(sp=dz, rep=oc)).start()

    def q_pair(n, _):
        with jax.named_scope("qtile"):
            for qi in (n, n + NZ // 2):
                q_tile(qi)
            for qi in (n, n + NZ // 2):
                send_out(qi)
        return 0

    lax.fori_loop(0, NZ // 2, q_pair, 0)

    with jax.named_scope("owait"):
        drain(out, orr)
    with jax.named_scope("sends"):
        give.wait_send()
        drain(wbuf.at[pl.ds(0, NP - 1), :, 0], zs)
        drain(wbuf.at[:, :, pl.ds(0, NX - 1)], xs)
        drain(hidden.at[pl.ds(0, half)], hs)
        drain(hidden.at[pl.ds(0, half)], gs)
        drain(buf.at[0], ds)
        drain(buf.at[0, pl.ds(0, 2 * span)], fs)

        q_self = r == z // (NZ // 2)
        for sem in (qs, os):

            @pl.when(q_self)
            def _():
                drain(qbuf.at[pl.ds(0, span - rows)], sem)

            @pl.when(jnp.logical_not(q_self))
            def _():
                drain(qbuf, sem)

        kv_self = q_self & (b == r)

        @pl.when(kv_self)
        def _():
            drain(buf.at[0, pl.ds(0, (2 * NH - 1) * prow)], ks)

        @pl.when(jnp.logical_not(kv_self))
        def _():
            drain(buf.at[0, pl.ds(0, 2 * NH * prow)], ks)


def on_device(
    hidden, queries, norm_gain, key_matrix, value_matrix, key_shift_bias, value_shift_bias,
    doc_lengths,
):
    NZ, NX = lax.axis_size("sp"), lax.axis_size("blk")
    NP = NZ // 2
    z, x = lax.axis_index("sp"), lax.axis_index("blk")
    rows, width = hidden.shape[1:]
    span = rows * NZ
    krows, kcols = key_matrix.shape
    heads = kcols // HEAD
    places = (x * span + (z // 2) * 2 * rows + jnp.arange(2 * rows)).astype(F32)
    lane = jnp.arange(HEAD)
    freq = (lane % (HEAD // 2)).astype(F32)
    inverse = jnp.exp(freq * (-2.0 * math.log(THETA_BASE) / HEAD))
    angles = places[:, None] * inverse[None, :]
    cos_t = jnp.cos(angles)
    sin_t = jnp.sin(angles) * jnp.where(lane < HEAD // 2, -1.0, 1.0).astype(F32)
    bias = jnp.stack([key_shift_bias, value_shift_bias]).astype(F32)
    HC = 4
    QN = queries.shape[2] // HEAD
    dma = pltpu.SemaphoreType.DMA
    vmem = pl.BlockSpec(memory_space=pltpu.VMEM)
    hbm = pl.BlockSpec(memory_space=pl.ANY)
    out = pl.pallas_call(
        functools.partial(body, NZ, NX),
        out_shape=jax.ShapeDtypeStruct((rows, queries.shape[2]), BF16),
        in_specs=[pl.BlockSpec(memory_space=pltpu.SMEM), hbm, hbm, vmem, hbm, hbm] + [vmem] * 3,
        out_specs=hbm,
        scratch_shapes=[
            pltpu.VMEM((NP, 2, NX, krows // NX, kcols), BF16),
            pltpu.VMEM((rows, width), BF16),
            pltpu.VMEM((rows, width), BF16),
            pltpu.VMEM((2 * rows, width), BF16),
            pltpu.VMEM((2 * rows, kcols), F32),
            pltpu.VMEM((heads, 2 * rows, HEAD), BF16),
            pltpu.VMEM((span, HEAD), BF16),
            pltpu.VMEM((2, 3 * span, HEAD), BF16),
            pltpu.VMEM((span, HEAD), BF16),
            dma(()), dma(()), dma(()), dma(()),
            dma(()), dma((2, NP // 2)),
            dma(()), dma((NP, 2, NX // 2)),
            dma(()), dma((HC,)), dma(()), dma(()),
            dma(()), dma(()),
            dma(()), dma((NP,)),
            dma(()), dma(()),
            dma(()), dma((2, NP)),
            dma(()), dma(()),
        ],
        compiler_params=pltpu.CompilerParams(
            collective_id=0, has_side_effects=True, vmem_limit_bytes=56 * 2**20
        ),
    )(
        doc_lengths, hidden[0], queries[0], norm_gain[None], key_matrix, value_matrix,
        bias, cos_t, sin_t,
    )
    return out[None]


def solution(mesh):
    in_specs = (
        P(("grp", "blk"), "sp", None),
        P(("grp", "blk"), "sp", "rep"),
        P(),
        P("sp", "rep"),
        P("sp", "rep"),
        P("rep"),
        P("rep"),
        P("grp"),
    )
    out_specs = P(("grp", "blk"), "sp", "rep")
    return jax.shard_map(
        on_device, mesh=mesh, in_specs=in_specs, out_specs=out_specs, check_vma=False
    )
```

```python
import functools
import math

import jax
import jax.numpy as jnp
from jax import lax
from jax.experimental import pallas as pl
from jax.experimental.pallas import tpu as pltpu
from jax.sharding import PartitionSpec as P

HEAD = 128
EPS_VALUE = 1e-06
THETA_BASE = 1000000.0
NEG_FILL = -1e30
KEY_TILE = 512
MESH = pl.DeviceIdType.MESH
F32 = jnp.float32
BF16 = jnp.bfloat16


def ring_offsets(n):
    order = [0]
    for k in range(1, n // 2):
        order += [-k, k]
    return order + [n // 2]


def near_first(count, ring):
    return [
        sorted(range(count), key=lambda c: min((c - k) % ring, (k - c) % ring)) for k in range(ring)
    ]


def pick(table, row, column):
    value = jnp.int32(table[0][column])
    for k in range(1, len(table)):
        value = jnp.where(row == k, table[k][column], value)
    return value


def body(
    NZ, NX,
    lengths, hidden, queries, gain, wk, wv, kb, vb, cos_t, sin_t,
    out,
    wbuf, hown, hbuf, nbuf, acc, kvown, qbuf, buf, obuf,
    pair_s, pair_r, rest_s, rest_r, own_s, hown_s, zs, zr, xs, xr, hs, hr, gs, gr, qs, qr,
    ks, kr, ps, ds, dr, fs, fr, os, orr,
):
    NP = NZ // 2
    ZH, XH = NP // 2, NX // 2
    z = lax.axis_index("sp")
    x = lax.axis_index("blk")
    r = lax.axis_index("rep")
    p = z // 2
    b = lax.rem(z, 2)
    rows = hidden.shape[0]
    half = rows // 2

    def mod(a, n):
        return lax.rem(a + 2 * n, n)

    def at(sp=None, blk=None, rep=None):
        return {
            "sp": z if sp is None else sp,
            "blk": x if blk is None else blk,
            "rep": r if rep is None else rep,
        }

    def remote(src, dst, ss, rs, dev):
        return pltpu.make_async_remote_copy(
            src_ref=src, dst_ref=dst, send_sem=ss, recv_sem=rs,
            device_id=dev, device_id_type=MESH,
        )

    def drain(ref, sem):
        pltpu.make_async_copy(ref, ref, sem).wait()

    def signal(sem, dev):
        pl.semaphore_signal(sem, inc=1, device_id=dev, device_id_type=MESH)

    barrier = pltpu.get_barrier_semaphore()
    for j in range(1, 2 * NZ):
        other = mod(2 * z + r + j, 2 * NZ)
        signal(barrier, at(sp=other // 2, rep=lax.rem(other, 2)))
    for dx in (1, -1):
        signal(barrier, at(blk=mod(x + dx, NX)))

    partner = z + 1 - 2 * b
    own_slot = wbuf.at[p, b]

    @pl.when(b == 0)
    def _():
        pltpu.make_async_copy(wk, own_slot, own_s).start()

    @pl.when(b == 1)
    def _():
        pltpu.make_async_copy(wv, own_slot, own_s).start()

    pltpu.make_async_copy(hidden, hown, hown_s).start()
    pl.semaphore_wait(barrier, 2 * NZ + 1)

    def give(k, ss, rs):
        sl = mod(x + k, NX)

        @pl.when(b == 0)
        def _():
            remote(wv.at[sl], wbuf.at[p, b, sl], ss, rs, at(sp=partner)).start()

        @pl.when(b == 1)
        def _():
            remote(wk.at[sl], wbuf.at[p, b, sl], ss, rs, at(sp=partner)).start()

    give(0, pair_s, pair_r)

    items = [mod(p + o, NP) for o in ring_offsets(NP)]

    def z_send(h, d):
        item = mod(p - (h - 1) if d == 0 else p + (h - 1), NP)
        ref = wbuf.at[item, :, x] if h < ZH else wbuf.at[item, d, x]
        to = mod(z + 2 if d == 0 else z - 2, NZ)
        return remote(ref, ref, zs, zr.at[d, h - 1], at(sp=to))

    def z_recv(h, d):
        item = mod(p - h if d == 0 else p + h, NP)
        ref = wbuf.at[item, :, x] if h < ZH else wbuf.at[item, d, x]
        return remote(ref, ref, zs, zr.at[d, h - 1], at(sp=mod(z + 2, NZ)))

    def x_send(i, h, d):
        sl = mod(x - (h - 1) if d == 0 else x + (h - 1), NX)
        ref = wbuf.at[items[i], :, sl] if h < XH else wbuf.at[items[i], d, sl]
        to = mod(x + 1 if d == 0 else x - 1, NX)
        return remote(ref, ref, xs, xr.at[i, d, h - 1], at(blk=to))

    def x_recv(i, h, d):
        sl = mod(x - h if d == 0 else x + h, NX)
        ref = wbuf.at[items[i], :, sl] if h < XH else wbuf.at[items[i], d, sl]
        return remote(ref, ref, xs, xr.at[i, d, h - 1], at(blk=mod(x + 1, NX)))

    HC = hr.shape[0]
    hrows = half // HC

    def h_send(k):
        ref_rows = pl.ds(pl.multiple_of(r * half + k * hrows, hrows), hrows)
        return remote(hidden.at[ref_rows], hbuf.at[ref_rows], hs, hr.at[k], at(sp=partner))

    def h_relay(k):
        ref_rows = pl.ds(pl.multiple_of(r * half + k * hrows, hrows), hrows)
        return remote(hbuf.at[ref_rows], hbuf.at[ref_rows], gs, gr, at(rep=1 - r))

    QN = queries.shape[1] // HEAD

    def q_case(j):
        chip, dc = lax.rem(p + j // 2, QN // 2), j % 2
        hl = 2 * chip + dc
        dz = r * (QN // 2) + chip
        src = queries.at[:, pl.ds(pl.multiple_of(hl * HEAD, HEAD), HEAD)]
        dst = qbuf.at[pl.ds(pl.multiple_of(z * rows, rows), rows)]
        return src, dst, at(sp=dz, rep=dc), (dz == z) & (dc == r)

    def start_q(j):
        src, dst, dev, self_case = q_case(j)

        @pl.when(self_case)
        def _():
            pltpu.make_async_copy(src, dst, qr).start()

        @pl.when(jnp.logical_not(self_case))
        def _():
            remote(src, dst, qs, qr, dev).start()

    def norm_into(src, row0):
        step = 16

        def one(k, _):
            at_rows = pl.ds(pl.multiple_of(k * step, step), step)
            v = src[at_rows, :].astype(F32)
            scale = lax.rsqrt(jnp.mean(v * v, axis=1, keepdims=True) + EPS_VALUE)
            nbuf[pl.ds(pl.multiple_of(row0 + k * step, step), step), :] = (
                v * scale * gain[...]
            ).astype(BF16)
            return 0

        lax.fori_loop(0, rows // step, one, 0)

    WK = wbuf.shape[1] * wbuf.shape[2] * wbuf.shape[3]

    def dot_item(i, first):
        lhs = nbuf[:, pl.ds(pl.multiple_of(items[i] * WK, WK), WK)]
        w = wbuf[items[i]].reshape(WK, wbuf.shape[4])
        d = jnp.dot(lhs, w, preferred_element_type=F32)
        if first:
            acc[...] = d
        else:
            acc[...] += d

    def first_hops(c):
        ref = wbuf.at[p, c, x]
        for d in (0, 1):
            to = mod(z + 2 if d == 0 else z - 2, NZ)
            remote(ref, ref, zs, zr.at[d, 0], at(sp=to)).start()

    pltpu.make_async_copy(wk, own_slot, own_s).wait()
    first_hops(b)
    drain(wbuf.at[p, 1 - b, x], pair_r)
    first_hops(1 - b)
    starts = [None, 1]
    for i in range(2, NP):
        starts.append(max((i + 1) // 2, starts[-1] + (i > 2)))
    last = starts[-1] + XH
    done_dots = 0
    order = list(range(1, NP)) + [0]
    q_next = 0
    q_ticks = [0] * (ZH - 1) + [2, 2, 3, 3, 3] + [0] * last
    q_ticks[2 * ZH] = QN - sum(q_ticks)
    for t in range(last + 1):
        with jax.named_scope(f"t{t}"):
            for h in range(XH, 0, -1):
                if h == 1:
                    if 1 <= t <= ZH:
                        for d in (0, 1):
                            z_recv(t, d).wait_recv()
                    if 0 < t < ZH:
                        for d in (0, 1):
                            z_send(t + 1, d).start()
                for i in range(1, NP):
                    if t == starts[i] + h - 1:
                        for d in (0, 1):
                            if h > 1:
                                x_recv(i, h - 1, d).wait_recv()
                            x_send(i, h, d).start()
            if t < HC:
                h_send(t).start()
            if t == 0:
                pltpu.make_async_copy(hidden, hown, hown_s).wait()
                norm_into(hown, b * rows)
            if t in (ZH, ZH + 1):
                for k in range(1, NX):
                    if (k <= NX // 2) == (t == ZH):
                        give(k, rest_s, rest_r)
            for _ in range(q_ticks[t]):
                start_q(q_next)
                q_next += 1
            if 3 <= t < HC + 3:
                h_send(t - 3).wait_recv()
                h_relay(t - 3).start()
            if t == HC + 3:
                drain(hbuf.at[pl.ds(pl.multiple_of((1 - r) * half, half), half)], gr)
                norm_into(hbuf, (1 - b) * rows)
            if t >= HC + 3:
                for _ in range(2 if t < last else NP):
                    if done_dots < NP - 1 and starts[order[done_dots]] + XH <= t:
                        for d in (0, 1):
                            x_recv(order[done_dots], XH, d).wait_recv()
                        dot_item(order[done_dots], done_dots == 0)
                        done_dots += 1
            if t == last - 2:
                drain(wbuf.at[p, 1 - b, pl.ds(0, NX - 1)], rest_r)
                dot_item(0, False)
    assert done_dots == NP - 1

    NH = kvown.shape[0]
    for j in range(NH):
        cols = slice(j * HEAD, (j + 1) * HEAD)

        @pl.when(b == 0)
        def _():
            y = acc[:, cols] + kb[cols].astype(F32).reshape(1, HEAD)
            kvown[j] = (y * cos_t[...] + pltpu.roll(y, HEAD // 2, 1) * sin_t[...]).astype(BF16)

        @pl.when(b == 1)
        def _():
            kvown[j] = (acc[:, cols] + vb[cols].astype(F32).reshape(1, HEAD)).astype(BF16)

    prow = 2 * rows
    span = rows * NZ

    def unit(a, q):
        return pl.ds(pl.multiple_of((2 - a) * span + q * prow, prow), prow)

    kv_heads = [pick(near_first(NH, NP), mod(p - NH * r, NP), k) for k in range(NH)]

    def kv_case(k):
        j = kv_heads[k]
        dz = 2 * (NH * r + j) + lax.rem(p, 2)
        return kvown.at[j], buf.at[b, unit(0, p)], at(sp=dz, rep=b), (dz == z) & (b == r)

    def start_kv(k):
        src, dst, dev, self_case = kv_case(k)

        @pl.when(self_case)
        def _():
            pltpu.make_async_copy(src, dst, kr.at[p]).start()

        @pl.when(jnp.logical_not(self_case))
        def _():
            remote(src, dst, ks, kr.at[p], dev).start()

    for k in range(NH):
        start_kv(k)

    def relay(a, q):
        here = buf.at[r, unit(a, q)]
        if a == 0:
            remote(here, here, ks, kr.at[q], at()).wait_recv()
        else:
            remote(here, here, fs, fr.at[a - 1, q], at()).wait_recv()
        if a == 0:

            @pl.when(lax.rem(q, 2) == b)
            def _():
                remote(here, here, ps, kr.at[q], at(sp=partner)).start()

        remote(here, here, ds, dr, at(rep=1 - r)).start()
        if a < 2:
            there = buf.at[r, unit(a + 1, q)]
            remote(here, there, fs, fr.at[a, q], at(blk=mod(x + 1, NX))).start()

    for i in range(NP + 4):
        with jax.named_scope(f"relay{i}"):
            for a in (0, 1, 2):
                if 0 <= i - 2 * a < NP:
                    relay(a, items[i - 2 * a])
            if i >= 6 and q_next < QN:
                start_q(q_next)
                q_next += 1
    assert q_next == QN
    with jax.named_scope("relayed"):
        drain(buf.at[1 - r], dr)
        drain(qbuf, qr)

    KT = KEY_TILE // rows
    factor = math.log2(math.e) / math.sqrt(HEAD)
    ones = jnp.ones((KEY_TILE, HEAD), BF16)
    oc = z // (NZ // 2)
    olane = lax.rem(2 * z + r, QN)
    odst = out.at[:, pl.ds(pl.multiple_of(olane * HEAD, HEAD), HEAD)]

    def q_tile(qi):
        q = qbuf[pl.ds(pl.multiple_of(qi * rows, rows), rows), :]
        first = x * span + qi * rows
        pos = first + lax.broadcasted_iota(jnp.int32, (rows, HEAD), 0)
        lo = jnp.zeros((rows, HEAD), jnp.int32)
        end = jnp.int32(0)
        for d in range(lengths.shape[0]):
            end = end + lengths[d]
            lo = jnp.where(pos >= end, end, lo)
        lo = lo - first
        m = None
        for back in range(2 * NZ // KT + 1):
            n = rows if back == 0 else KEY_TILE
            at_rows = pl.ds(pl.multiple_of(2 * span + qi * rows - back * KEY_TILE, rows), n)
            s = lax.dot_general(
                q, buf[0, at_rows, :], (((1,), (1,)), ((), ())), preferred_element_type=F32
            )
            col = lax.broadcasted_iota(jnp.int32, (rows, n), 1)
            low = lo + back * KEY_TILE
            seen = col >= jnp.concatenate([low] * (n // HEAD), axis=1)
            if back == 0:
                seen = seen & (col <= lax.broadcasted_iota(jnp.int32, (rows, n), 0))
            s = jnp.where(seen, s, NEG_FILL)
            top = jnp.broadcast_to(jnp.max(s, axis=1, keepdims=True), (rows, HEAD))
            m_new = top if m is None else jnp.maximum(m, top)
            w = jnp.exp2((s - jnp.concatenate([m_new] * (n // HEAD), axis=1)) * factor).astype(BF16)
            vv = jnp.concatenate([buf[1, at_rows, :], ones[:n]], axis=1)
            pv = jnp.dot(w, vv, preferred_element_type=F32)
            if m is None:
                total = pv
            else:
                alpha = jnp.exp2((m - m_new) * factor)
                total = total * jnp.concatenate([alpha, alpha], axis=1) + pv
            m = m_new
        obuf[pl.ds(pl.multiple_of(qi * rows, rows), rows), :] = (
            total[:, :HEAD] / total[:, HEAD:]
        ).astype(BF16)

    def send_out(dz):
        src = obuf.at[pl.ds(pl.multiple_of(dz * rows, rows), rows)]
        self_case = (dz == z) & (oc == r)

        @pl.when(self_case)
        def _():
            pltpu.make_async_copy(src, odst, orr).start()

        @pl.when(jnp.logical_not(self_case))
        def _():
            remote(src, odst, os, orr, at(sp=dz, rep=oc)).start()

    def q_pair(n, _):
        with jax.named_scope("qtile"):
            tiles = (lax.rem(z + NZ // 2 - n + NZ, NZ), lax.rem(z + NZ // 2 + 1 + n, NZ))
            for qi in tiles:
                q_tile(qi)
            for qi in tiles:
                send_out(qi)
        return 0

    lax.fori_loop(0, NZ // 2, q_pair, 0)

    with jax.named_scope("owait"):
        drain(out, orr)
    with jax.named_scope("sends"):
        drain(wbuf.at[p, b, x], pair_s)
        drain(wbuf.at[p, b, pl.ds(0, NX - 1)], rest_s)
        drain(wbuf.at[pl.ds(0, NP - 1), :, 0], zs)
        drain(wbuf.at[pl.ds(0, NP - 1), :, pl.ds(0, NX - 1)], xs)
        drain(hidden.at[pl.ds(0, half)], hs)
        drain(hidden.at[pl.ds(0, half)], gs)
        drain(buf.at[0], ds)
        drain(buf.at[0, pl.ds(0, NH * prow)], ps)
        drain(buf.at[0, pl.ds(0, 2 * span)], fs)

        q_self = r == z // (NZ // 2)
        for sem in (qs, os):

            @pl.when(q_self)
            def _():
                drain(qbuf.at[pl.ds(0, span - rows)], sem)

            @pl.when(jnp.logical_not(q_self))
            def _():
                drain(qbuf, sem)

        kv_self = q_self & (b == r) & (lax.rem(p, 2) == b)

        @pl.when(kv_self)
        def _():
            drain(buf.at[0, pl.ds(0, (NH - 1) * prow)], ks)

        @pl.when(jnp.logical_not(kv_self))
        def _():
            drain(buf.at[0, pl.ds(0, NH * prow)], ks)


def on_device(
    hidden, queries, norm_gain, key_matrix, value_matrix, key_shift_bias, value_shift_bias,
    doc_lengths,
):
    NZ, NX = lax.axis_size("sp"), lax.axis_size("blk")
    NP = NZ // 2
    z, x = lax.axis_index("sp"), lax.axis_index("blk")
    rows, width = hidden.shape[1:]
    span = rows * NZ
    krows, kcols = key_matrix.shape
    heads = kcols // HEAD
    places = (x * span + (z // 2) * 2 * rows + jnp.arange(2 * rows)).astype(F32)
    lane = jnp.arange(HEAD)
    freq = (lane % (HEAD // 2)).astype(F32)
    inverse = jnp.exp(freq * (-2.0 * math.log(THETA_BASE) / HEAD))
    angles = places[:, None] * inverse[None, :]
    cos_t = jnp.cos(angles)
    sin_t = jnp.sin(angles) * jnp.where(lane < HEAD // 2, -1.0, 1.0).astype(F32)
    HC = 4
    QN = queries.shape[2] // HEAD
    dma = pltpu.SemaphoreType.DMA
    vmem = pl.BlockSpec(memory_space=pltpu.VMEM)
    hbm = pl.BlockSpec(memory_space=pl.ANY)
    out = pl.pallas_call(
        functools.partial(body, NZ, NX),
        out_shape=jax.ShapeDtypeStruct((rows, queries.shape[2]), BF16),
        in_specs=[pl.BlockSpec(memory_space=pltpu.SMEM), hbm, hbm, vmem, hbm, hbm] + [vmem] * 4,
        out_specs=hbm,
        scratch_shapes=[
            pltpu.VMEM((NP, 2, NX, krows // NX, kcols), BF16),
            pltpu.VMEM((rows, width), BF16),
            pltpu.VMEM((rows, width), BF16),
            pltpu.VMEM((2 * rows, width), BF16),
            pltpu.VMEM((2 * rows, kcols), F32),
            pltpu.VMEM((heads, 2 * rows, HEAD), BF16),
            pltpu.VMEM((span, HEAD), BF16),
            pltpu.VMEM((2, 3 * span, HEAD), BF16),
            pltpu.VMEM((span, HEAD), BF16),
            dma(()), dma(()), dma(()), dma(()), dma(()), dma(()),
            dma(()), dma((2, NP // 2)),
            dma(()), dma((NP, 2, NX // 2)),
            dma(()), dma((HC,)), dma(()), dma(()),
            dma(()), dma(()),
            dma(()), dma((NP,)), dma(()),
            dma(()), dma(()),
            dma(()), dma((2, NP)),
            dma(()), dma(()),
        ],
        compiler_params=pltpu.CompilerParams(
            collective_id=0, has_side_effects=True, vmem_limit_bytes=56 * 2**20
        ),
    )(
        doc_lengths, hidden[0], queries[0], norm_gain[None],
        key_matrix.reshape(NX, krows // NX, kcols), value_matrix.reshape(NX, krows // NX, kcols),
        key_shift_bias, value_shift_bias, cos_t, sin_t,
    )
    return out[None]


def solution(mesh):
    in_specs = (
        P(("grp", "blk"), "sp", None),
        P(("grp", "blk"), "sp", "rep"),
        P(),
        P("sp", "rep"),
        P("sp", "rep"),
        P("rep"),
        P("rep"),
        P("grp"),
    )
    out_specs = P(("grp", "blk"), "sp", "rep")
    return jax.shard_map(
        on_device, mesh=mesh, in_specs=in_specs, out_specs=out_specs, check_vma=False
    )
```

```python
import functools
import math

import jax
import jax.numpy as jnp
from jax import lax
from jax.experimental import pallas as pl
from jax.experimental.pallas import tpu as pltpu
from jax.sharding import PartitionSpec as P

HEAD = 128
EPS_VALUE = 1e-06
THETA_BASE = 1000000.0
NEG_FILL = -1e30
KEY_TILE = 512
MESH = pl.DeviceIdType.MESH
F32 = jnp.float32
BF16 = jnp.bfloat16


def ring_offsets(n):
    order = [0]
    for k in range(1, n // 2):
        order += [-k, k]
    return order + [n // 2]


def near_first(count, ring):
    return [
        sorted(range(count), key=lambda c: min((c - k) % ring, (k - c) % ring)) for k in range(ring)
    ]


def pick(table, row, column):
    value = jnp.int32(table[0][column])
    for k in range(1, len(table)):
        value = jnp.where(row == k, table[k][column], value)
    return value


def body(
    NZ, NX,
    lengths, hidden, queries, gain, wk, wv, kb, vb, cos_t, sin_t,
    out,
    wbuf, hown, hbuf, nbuf, acc, kvown, qbuf, buf, obuf,
    pair_s, pair_r, rest_s, rest_r, own_s, hown_s, zs, zr, xs, xr, hs, hr, gs, gr, qs, qr,
    ks, kr, ps, ds, dr, fs, fr, os, orr,
):
    NP = NZ // 2
    ZH, XH = NP // 2, NX // 2
    z = lax.axis_index("sp")
    x = lax.axis_index("blk")
    r = lax.axis_index("rep")
    p = z // 2
    b = lax.rem(z, 2)
    rows = hidden.shape[0]
    half = rows // 2

    def mod(a, n):
        return lax.rem(a + 2 * n, n)

    def at(sp=None, blk=None, rep=None):
        return {
            "sp": z if sp is None else sp,
            "blk": x if blk is None else blk,
            "rep": r if rep is None else rep,
        }

    def remote(src, dst, ss, rs, dev):
        return pltpu.make_async_remote_copy(
            src_ref=src, dst_ref=dst, send_sem=ss, recv_sem=rs,
            device_id=dev, device_id_type=MESH,
        )

    def drain(ref, sem):
        pltpu.make_async_copy(ref, ref, sem).wait()

    def signal(sem, dev):
        pl.semaphore_signal(sem, inc=1, device_id=dev, device_id_type=MESH)

    barrier = pltpu.get_barrier_semaphore()
    for j in range(1, 2 * NZ):
        other = mod(2 * z + r + j, 2 * NZ)
        signal(barrier, at(sp=other // 2, rep=lax.rem(other, 2)))
    for dx in (1, -1):
        signal(barrier, at(blk=mod(x + dx, NX)))

    partner = z + 1 - 2 * b
    own_slot = wbuf.at[p, b]

    @pl.when(b == 0)
    def _():
        pltpu.make_async_copy(wk, own_slot, own_s).start()

    @pl.when(b == 1)
    def _():
        pltpu.make_async_copy(wv, own_slot, own_s).start()

    pltpu.make_async_copy(hidden, hown, hown_s).start()
    pl.semaphore_wait(barrier, 2 * NZ + 1)

    def give(k, ss, rs):
        sl = mod(x + k, NX)

        @pl.when(b == 0)
        def _():
            remote(wv.at[sl], wbuf.at[p, b, sl], ss, rs, at(sp=partner)).start()

        @pl.when(b == 1)
        def _():
            remote(wk.at[sl], wbuf.at[p, b, sl], ss, rs, at(sp=partner)).start()

    give(0, pair_s, pair_r)

    items = [mod(p + o, NP) for o in ring_offsets(NP)]

    def z_send(h, d):
        item = mod(p - (h - 1) if d == 0 else p + (h - 1), NP)
        ref = wbuf.at[item, :, x] if h < ZH else wbuf.at[item, d, x]
        to = mod(z + 2 if d == 0 else z - 2, NZ)
        return remote(ref, ref, zs, zr.at[d, h - 1], at(sp=to))

    def z_recv(h, d):
        item = mod(p - h if d == 0 else p + h, NP)
        ref = wbuf.at[item, :, x] if h < ZH else wbuf.at[item, d, x]
        return remote(ref, ref, zs, zr.at[d, h - 1], at(sp=mod(z + 2, NZ)))

    def x_send(i, h, d):
        sl = mod(x - (h - 1) if d == 0 else x + (h - 1), NX)
        ref = wbuf.at[items[i], :, sl] if h < XH else wbuf.at[items[i], d, sl]
        to = mod(x + 1 if d == 0 else x - 1, NX)
        return remote(ref, ref, xs, xr.at[i, d, h - 1], at(blk=to))

    def x_recv(i, h, d):
        sl = mod(x - h if d == 0 else x + h, NX)
        ref = wbuf.at[items[i], :, sl] if h < XH else wbuf.at[items[i], d, sl]
        return remote(ref, ref, xs, xr.at[i, d, h - 1], at(blk=mod(x + 1, NX)))

    HC = hr.shape[0]
    hrows = half // HC

    def h_send(k):
        ref_rows = pl.ds(pl.multiple_of(r * half + k * hrows, hrows), hrows)
        return remote(hidden.at[ref_rows], hbuf.at[ref_rows], hs, hr.at[k], at(sp=partner))

    def h_relay(k):
        ref_rows = pl.ds(pl.multiple_of(r * half + k * hrows, hrows), hrows)
        return remote(hbuf.at[ref_rows], hbuf.at[ref_rows], gs, gr, at(rep=1 - r))

    QN = queries.shape[1] // HEAD

    def q_case(j):
        chip, dc = lax.rem(p + j // 2, QN // 2), j % 2
        hl = 2 * chip + dc
        dz = r * (QN // 2) + chip
        src = queries.at[:, pl.ds(pl.multiple_of(hl * HEAD, HEAD), HEAD)]
        dst = qbuf.at[pl.ds(pl.multiple_of(z * rows, rows), rows)]
        return src, dst, at(sp=dz, rep=dc), (dz == z) & (dc == r)

    def start_q(j):
        src, dst, dev, self_case = q_case(j)

        @pl.when(self_case)
        def _():
            pltpu.make_async_copy(src, dst, qr).start()

        @pl.when(jnp.logical_not(self_case))
        def _():
            remote(src, dst, qs, qr, dev).start()

    def norm_into(src, row0):
        step = 16

        def one(k, _):
            at_rows = pl.ds(pl.multiple_of(k * step, step), step)
            v = src[at_rows, :].astype(F32)
            scale = lax.rsqrt(jnp.mean(v * v, axis=1, keepdims=True) + EPS_VALUE)
            nbuf[pl.ds(pl.multiple_of(row0 + k * step, step), step), :] = (
                v * scale * gain[...]
            ).astype(BF16)
            return 0

        lax.fori_loop(0, rows // step, one, 0)

    WK = wbuf.shape[1] * wbuf.shape[2] * wbuf.shape[3]

    def dot_item(i, first):
        lhs = nbuf[:, pl.ds(pl.multiple_of(items[i] * WK, WK), WK)]
        w = wbuf[items[i]].reshape(WK, wbuf.shape[4])
        d = jnp.dot(lhs, w, preferred_element_type=F32)
        if first:
            acc[...] = d
        else:
            acc[...] += d

    def first_hops(c):
        ref = wbuf.at[p, c, x]
        for d in (0, 1):
            to = mod(z + 2 if d == 0 else z - 2, NZ)
            remote(ref, ref, zs, zr.at[d, 0], at(sp=to)).start()

    pltpu.make_async_copy(wk, own_slot, own_s).wait()
    first_hops(b)
    drain(wbuf.at[p, 1 - b, x], pair_r)
    first_hops(1 - b)
    starts = [None, 1]
    for i in range(2, NP):
        starts.append(max((i + 1) // 2, starts[-1] + (i > 2)))
    last = starts[-1] + XH
    done_dots = 0
    order = list(range(1, NP)) + [0]
    q_next = 0
    q_ticks = [0] * (ZH - 1) + [2, 2, 3, 3, 3] + [0] * last
    q_ticks[2 * ZH] = QN - sum(q_ticks)
    for t in range(last + 1):
        with jax.named_scope(f"t{t}"):
            for h in range(XH, 0, -1):
                if h == 1:
                    if 1 <= t <= ZH:
                        for d in (0, 1):
                            z_recv(t, d).wait_recv()
                    if 0 < t < ZH:
                        for d in (0, 1):
                            z_send(t + 1, d).start()
                for i in range(1, NP):
                    if t == starts[i] + h - 1:
                        for d in (0, 1):
                            if h > 1:
                                x_recv(i, h - 1, d).wait_recv()
                            x_send(i, h, d).start()
            if t < HC:
                h_send(t).start()
            if t == 0:
                pltpu.make_async_copy(hidden, hown, hown_s).wait()
                norm_into(hown, b * rows)
            if t in (ZH, ZH + 1):
                for k in range(1, NX):
                    if (k <= NX // 2) == (t == ZH):
                        give(k, rest_s, rest_r)
            for _ in range(q_ticks[t]):
                start_q(q_next)
                q_next += 1
            if 3 <= t < HC + 3:
                h_send(t - 3).wait_recv()
                h_relay(t - 3).start()
            if t == HC + 3:
                drain(hbuf.at[pl.ds(pl.multiple_of((1 - r) * half, half), half)], gr)
                norm_into(hbuf, (1 - b) * rows)
            if t >= HC + 3:
                for _ in range(2 if t < last else NP):
                    if done_dots < NP - 1 and starts[order[done_dots]] + XH <= t:
                        for d in (0, 1):
                            x_recv(order[done_dots], XH, d).wait_recv()
                        dot_item(order[done_dots], done_dots == 0)
                        done_dots += 1
            if t == last - 2:
                drain(wbuf.at[p, 1 - b, pl.ds(0, NX - 1)], rest_r)
                dot_item(0, False)
    assert done_dots == NP - 1

    NH = kvown.shape[0]
    for j in range(NH):
        cols = slice(j * HEAD, (j + 1) * HEAD)

        @pl.when(b == 0)
        def _():
            y = acc[:, cols] + kb[cols].astype(F32).reshape(1, HEAD)
            kvown[j] = (y * cos_t[...] + pltpu.roll(y, HEAD // 2, 1) * sin_t[...]).astype(BF16)

        @pl.when(b == 1)
        def _():
            kvown[j] = (acc[:, cols] + vb[cols].astype(F32).reshape(1, HEAD)).astype(BF16)

    prow = 2 * rows
    span = rows * NZ

    def unit(a, q):
        return pl.ds(pl.multiple_of((2 - a) * span + q * prow, prow), prow)

    kv_heads = [pick(near_first(NH, NP), mod(p - NH * r, NP), k) for k in range(NH)]

    def kv_case(k):
        j = kv_heads[k]
        dz = 2 * (NH * r + j) + lax.rem(p, 2)
        return kvown.at[j], buf.at[b, unit(0, p)], at(sp=dz, rep=b), (dz == z) & (b == r)

    def start_kv(k):
        src, dst, dev, self_case = kv_case(k)

        @pl.when(self_case)
        def _():
            pltpu.make_async_copy(src, dst, kr.at[p]).start()

        @pl.when(jnp.logical_not(self_case))
        def _():
            remote(src, dst, ks, kr.at[p], dev).start()

    for k in range(NH):
        start_kv(k)

    def relay(a, q):
        here = buf.at[r, unit(a, q)]
        if a == 0:
            remote(here, here, ks, kr.at[q], at()).wait_recv()
        else:
            remote(here, here, fs, fr.at[a - 1, q], at()).wait_recv()
        came_here = lax.rem(q, 2) == b
        if a != 1:

            @pl.when(came_here)
            def _():
                remote(here, here, ps, kr.at[q] if a == 0 else fr.at[1, q], at(sp=partner)).start()

        remote(here, here, ds, dr, at(rep=1 - r)).start()
        if a < 2:

            @pl.when(came_here | (a == 0))
            def _():
                there = buf.at[r, unit(a + 1, q)]
                remote(here, there, fs, fr.at[a, q], at(blk=mod(x + 1, NX))).start()

    offs = ring_offsets(NP)
    split = [[o for o in offs if o % 2 == parity] for parity in (0, 1)]
    orders = []
    for here, other in (split, split[::-1]):
        order = here[:1]
        for k in range(1, len(here)):
            order += [here[k], other[k - 1]]
        orders.append(order + other[-1:])
    same = b == lax.rem(p, 2)
    pairs = [mod(p + jnp.where(same, o, e), NP) for o, e in zip(*orders)]
    for i in range(NP + 4):
        with jax.named_scope(f"relay{i}"):
            for a in (0, 1, 2):
                if 0 <= i - 2 * a < NP:
                    relay(a, pairs[i - 2 * a])
            if i >= 6 and q_next < QN:
                start_q(q_next)
                q_next += 1
    assert q_next == QN
    with jax.named_scope("relayed"):
        drain(buf.at[1 - r], dr)
        drain(qbuf, qr)

    KT = KEY_TILE // rows
    factor = math.log2(math.e) / math.sqrt(HEAD)
    ones = jnp.ones((KEY_TILE, HEAD), BF16)
    oc = z // (NZ // 2)
    olane = lax.rem(2 * z + r, QN)
    odst = out.at[:, pl.ds(pl.multiple_of(olane * HEAD, HEAD), HEAD)]

    def q_tile(qi):
        q = qbuf[pl.ds(pl.multiple_of(qi * rows, rows), rows), :]
        first = x * span + qi * rows
        pos = first + lax.broadcasted_iota(jnp.int32, (rows, HEAD), 0)
        lo = jnp.zeros((rows, HEAD), jnp.int32)
        end = jnp.int32(0)
        for d in range(lengths.shape[0]):
            end = end + lengths[d]
            lo = jnp.where(pos >= end, end, lo)
        lo = lo - first
        m = None
        for back in range(2 * NZ // KT + 1):
            n = rows if back == 0 else KEY_TILE
            at_rows = pl.ds(pl.multiple_of(2 * span + qi * rows - back * KEY_TILE, rows), n)
            s = lax.dot_general(
                q, buf[0, at_rows, :], (((1,), (1,)), ((), ())), preferred_element_type=F32
            )
            col = lax.broadcasted_iota(jnp.int32, (rows, n), 1)
            low = lo + back * KEY_TILE
            seen = col >= jnp.concatenate([low] * (n // HEAD), axis=1)
            if back == 0:
                seen = seen & (col <= lax.broadcasted_iota(jnp.int32, (rows, n), 0))
            s = jnp.where(seen, s, NEG_FILL)
            top = jnp.broadcast_to(jnp.max(s, axis=1, keepdims=True), (rows, HEAD))
            m_new = top if m is None else jnp.maximum(m, top)
            w = jnp.exp2((s - jnp.concatenate([m_new] * (n // HEAD), axis=1)) * factor).astype(BF16)
            vv = jnp.concatenate([buf[1, at_rows, :], ones[:n]], axis=1)
            pv = jnp.dot(w, vv, preferred_element_type=F32)
            if m is None:
                total = pv
            else:
                alpha = jnp.exp2((m - m_new) * factor)
                total = total * jnp.concatenate([alpha, alpha], axis=1) + pv
            m = m_new
        obuf[pl.ds(pl.multiple_of(qi * rows, rows), rows), :] = (
            total[:, :HEAD] / total[:, HEAD:]
        ).astype(BF16)

    def send_out(dz):
        src = obuf.at[pl.ds(pl.multiple_of(dz * rows, rows), rows)]
        self_case = (dz == z) & (oc == r)

        @pl.when(self_case)
        def _():
            pltpu.make_async_copy(src, odst, orr).start()

        @pl.when(jnp.logical_not(self_case))
        def _():
            remote(src, odst, os, orr, at(sp=dz, rep=oc)).start()

    def q_pair(n, _):
        with jax.named_scope("qtile"):
            tiles = (lax.rem(z + NZ // 2 - n + NZ, NZ), lax.rem(z + NZ // 2 + 1 + n, NZ))
            for qi in tiles:
                q_tile(qi)
            for qi in tiles:
                send_out(qi)
        return 0

    lax.fori_loop(0, NZ // 2, q_pair, 0)

    with jax.named_scope("owait"):
        drain(out, orr)
    with jax.named_scope("sends"):
        drain(wbuf.at[p, b, x], pair_s)
        drain(wbuf.at[p, b, pl.ds(0, NX - 1)], rest_s)
        drain(wbuf.at[pl.ds(0, NP - 1), :, 0], zs)
        drain(wbuf.at[pl.ds(0, NP - 1), :, pl.ds(0, NX - 1)], xs)
        drain(hidden.at[pl.ds(0, half)], hs)
        drain(hidden.at[pl.ds(0, half)], gs)
        drain(buf.at[0], ds)
        drain(buf.at[0, pl.ds(0, 2 * NH * prow)], ps)
        drain(buf.at[0, pl.ds(0, span + NH * prow)], fs)

        q_self = r == z // (NZ // 2)
        for sem in (qs, os):

            @pl.when(q_self)
            def _():
                drain(qbuf.at[pl.ds(0, span - rows)], sem)

            @pl.when(jnp.logical_not(q_self))
            def _():
                drain(qbuf, sem)

        kv_self = q_self & (b == r) & (lax.rem(p, 2) == b)

        @pl.when(kv_self)
        def _():
            drain(buf.at[0, pl.ds(0, (NH - 1) * prow)], ks)

        @pl.when(jnp.logical_not(kv_self))
        def _():
            drain(buf.at[0, pl.ds(0, NH * prow)], ks)


def on_device(
    hidden, queries, norm_gain, key_matrix, value_matrix, key_shift_bias, value_shift_bias,
    doc_lengths,
):
    NZ, NX = lax.axis_size("sp"), lax.axis_size("blk")
    NP = NZ // 2
    z, x = lax.axis_index("sp"), lax.axis_index("blk")
    rows, width = hidden.shape[1:]
    span = rows * NZ
    krows, kcols = key_matrix.shape
    heads = kcols // HEAD
    places = (x * span + (z // 2) * 2 * rows + jnp.arange(2 * rows)).astype(F32)
    lane = jnp.arange(HEAD)
    freq = (lane % (HEAD // 2)).astype(F32)
    inverse = jnp.exp(freq * (-2.0 * math.log(THETA_BASE) / HEAD))
    angles = places[:, None] * inverse[None, :]
    cos_t = jnp.cos(angles)
    sin_t = jnp.sin(angles) * jnp.where(lane < HEAD // 2, -1.0, 1.0).astype(F32)
    HC = 4
    QN = queries.shape[2] // HEAD
    dma = pltpu.SemaphoreType.DMA
    vmem = pl.BlockSpec(memory_space=pltpu.VMEM)
    hbm = pl.BlockSpec(memory_space=pl.ANY)
    out = pl.pallas_call(
        functools.partial(body, NZ, NX),
        out_shape=jax.ShapeDtypeStruct((rows, queries.shape[2]), BF16),
        in_specs=[pl.BlockSpec(memory_space=pltpu.SMEM), hbm, hbm, vmem, hbm, hbm] + [vmem] * 4,
        out_specs=hbm,
        scratch_shapes=[
            pltpu.VMEM((NP, 2, NX, krows // NX, kcols), BF16),
            pltpu.VMEM((rows, width), BF16),
            pltpu.VMEM((rows, width), BF16),
            pltpu.VMEM((2 * rows, width), BF16),
            pltpu.VMEM((2 * rows, kcols), F32),
            pltpu.VMEM((heads, 2 * rows, HEAD), BF16),
            pltpu.VMEM((span, HEAD), BF16),
            pltpu.VMEM((2, 3 * span, HEAD), BF16),
            pltpu.VMEM((span, HEAD), BF16),
            dma(()), dma(()), dma(()), dma(()), dma(()), dma(()),
            dma(()), dma((2, NP // 2)),
            dma(()), dma((NP, 2, NX // 2)),
            dma(()), dma((HC,)), dma(()), dma(()),
            dma(()), dma(()),
            dma(()), dma((NP,)), dma(()),
            dma(()), dma(()),
            dma(()), dma((2, NP)),
            dma(()), dma(()),
        ],
        compiler_params=pltpu.CompilerParams(
            collective_id=0, has_side_effects=True, vmem_limit_bytes=56 * 2**20
        ),
    )(
        doc_lengths, hidden[0], queries[0], norm_gain[None],
        key_matrix.reshape(NX, krows // NX, kcols), value_matrix.reshape(NX, krows // NX, kcols),
        key_shift_bias, value_shift_bias, cos_t, sin_t,
    )
    return out[None]


def solution(mesh):
    in_specs = (
        P(("grp", "blk"), "sp", None),
        P(("grp", "blk"), "sp", "rep"),
        P(),
        P("sp", "rep"),
        P("sp", "rep"),
        P("rep"),
        P("rep"),
        P("grp"),
    )
    out_specs = P(("grp", "blk"), "sp", "rep")
    return jax.shard_map(
        on_device, mesh=mesh, in_specs=in_specs, out_specs=out_specs, check_vma=False
    )
```
